32 devices in a mesh: groups: 2 (over y), seq: 4 (over z), tp: 4 (over x, core).
Axes of the slice: x: 2, y: 2, z: 4, core: 2. Of those that a mesh axis runs over, the one named last changes fastest.
Arguments:
- prompt_kv: bfloat16 [32768, 64, 128], P(('groups', 'seq', 'tp')), parts along dimension 0, may hold values from -6 to 6
- prompt_length: int32 [2], P('groups'), parts along dimension 0, may hold values from 8192 to 16384
- queries: bfloat16 [16, 4096], P('groups'), parts along dimension 0, may hold values from -6 to 6
- new_kv: bfloat16 [16, 16, 2, 128], P('groups'), parts along dimension 0, may hold values from -6 to 6
- k_cache: bfloat16 [256, 8192, 128], P(('groups', 'seq'), 'tp'), parts along dimension 0, may hold values from -6 to 6
- v_cache: bfloat16 [256, 8192, 128], P(('groups', 'seq'), 'tp'), parts along dimension 0, may hold values from -6 to 6
- lengths: int32 [16], P('groups'), parts along dimension 0, may hold values from 4097 to 8192
- slots: int32 [16], P('groups'), parts along dimension 0, may hold values from 0 to 7, each once
Outputs:
- prompt_owned: bfloat16 [32768, 64, 128], P(('groups', 'tp'), 'seq'), parts along dimension 0
- attended: bfloat16 [256, 256], P(('groups', 'seq')), parts along dimension 0
The draws below stay inside these ranges and needn't reach their ends.
There are 2 independent parts, one for each index of `groups`. The reference program is written for one: setup_inputs(seed, part) draws one part's arguments, and reference() takes and returns one part's arrays. A program takes and returns all parts, laid end to end along the dimension named above; each array names one. Nothing has to cross between parts.
Inputs may be any that keep to these rules, and one draw needn't show every extreme that they name: `slots`: each slot once.
All inputs are finite; a program needn't handle non-finite values.
Results may differ from the reference program's by a relative error of at most 0.0028.
Values may be sent and summed in bfloat16 or wider, within the bound.
No kernel may reach another device: no remote copies, remote signals or barrier semaphores. Data moves between devices by JAX's collectives and lax.ppermute only.
A program may use at most 128 MiB of HBM per device.

```python
import jax
import jax.numpy as jnp
from jax import lax

KVH = 16
QH = 32
HD = 128
RESIDENT = 8
CACHE_LEN = 8192
PROMPT = 16384
GROUP = 2
KV_ROWS = 64
PAIRS = 128
BLOCK = 1024
N_SEQ = 4
N_TP = 4


query_scale = 168.0 ** (-0.5)


cache_strength = 6.0


def common_pattern(key):
    signs = jax.random.bernoulli(jax.random.fold_in(key, 7101), 0.5, (HD,))
    return jnp.where(signs, 1.0, -1.0).astype(jnp.float32)


def aligned_strengths(key):
    picked = jax.random.randint(jax.random.fold_in(key, 7102), (RESIDENT,), 0, 8)
    target = 120.0 + 70.0 * picked.astype(jnp.float32)
    strength = target / (cache_strength * HD * query_scale)
    return jnp.where(picked < 4, strength, 0.0)


def draw_queries(key, part):
    plain = jnp.clip(jax.random.normal(jax.random.fold_in(key, 7201), (RESIDENT, QH * HD), jnp.float32), -6.0, 6.0)
    pattern = jnp.tile(common_pattern(key), QH)
    strength = aligned_strengths(key)
    plain = jnp.where(strength[:, None] > 0.0, strength[:, None] * pattern[None, :], plain)
    return plain.astype(jnp.bfloat16)


def draw_new_kv(key, part):
    plain = jnp.clip(jax.random.normal(jax.random.fold_in(key, 7301), (RESIDENT, KVH, 2, HD), jnp.float32), -6.0, 6.0)
    pattern = common_pattern(key)
    strength = aligned_strengths(key)
    safe = jnp.maximum(strength, 1.0)
    level = cache_strength - 2.0 / (safe * HD * query_scale)
    aligned = jnp.broadcast_to((level[:, None] * pattern[None, :])[:, None, :], (RESIDENT, KVH, HD))
    keys = jnp.where(strength[:, None, None] > 0.0, aligned, plain[:, :, 0, :])
    plain = jnp.stack([keys, plain[:, :, 1, :]], axis=2)
    return plain.astype(jnp.bfloat16)


def draw_k_cache(key, part):
    plain = jnp.clip(jax.random.normal(jax.random.fold_in(key, 7401), (PAIRS, CACHE_LEN, HD), jnp.float32), -6.0, 6.0)
    pattern = common_pattern(key)
    first = jnp.broadcast_to(cache_strength * pattern[None, None, :], (PAIRS, 1, HD))
    plain = jnp.concatenate([first, plain[:, 1:, :]], axis=1)
    return plain.astype(jnp.bfloat16)


def touch_ends(entries, key, low, largest):
    index_at = [jax.random.randint(jax.random.fold_in(key, axis), (), 0, length) for axis, length in enumerate(entries.shape)]
    widest = entries.shape.index(max(entries.shape))
    beside = index_at[:widest] + [(index_at[widest] + 1) % entries.shape[widest]] + index_at[widest + 1:]
    return entries.at[tuple(index_at)].set(low).at[tuple(beside)].set(largest)


def levels(stream_key, shape, shards, least, largest):
    factor_of = 1.0
    for dim, parts in shards:
        draws = jax.random.uniform(jax.random.fold_in(jax.random.fold_in(stream_key, 6), dim), (parts,), jnp.float32, least / len(shards), largest / len(shards))
        factor_of = factor_of * jnp.repeat(jnp.exp(draws), shape[dim] // parts).reshape((-1,) + (1,) * (len(shape) - 1 - dim))
    return factor_of


def gaussian(key, extent, spread, most, shards=(), kind=jnp.bfloat16):
    gain = levels(key, extent, shards, -0.22, 0.18) if shards else 1.0
    entries = jax.random.normal(key, extent, jnp.float32) * spread * gain
    return jnp.minimum(jnp.maximum(entries, -most), most).astype(kind)


def setup_inputs(seed: int = 0, part: int = 0) -> dict:
    key_list = jax.random.split(jax.random.key(seed), 9)
    part_keys = jax.random.split(jax.random.fold_in(key_list[8], part), 9)
    prompt_kv = gaussian(part_keys[0], (PROMPT, KV_ROWS, HD), 1.0, 6.0, ((0, 16),))
    prompt_length = jax.random.randint(part_keys[1], (1,), PROMPT // 2, PROMPT + 1).astype(jnp.int32)
    queries = draw_queries(jax.random.fold_in(jax.random.fold_in(key_list[8], part), 71), part)
    new_kv = draw_new_kv(jax.random.fold_in(jax.random.fold_in(key_list[8], part), 71), part)
    k_cache = draw_k_cache(jax.random.fold_in(jax.random.fold_in(key_list[8], part), 71), part)
    v_cache = gaussian(part_keys[5], (PAIRS, CACHE_LEN, HD), 1.0, 6.0, ((0, 4), (1, 4)))
    lengths = touch_ends(jax.random.randint(part_keys[6], (RESIDENT,), CACHE_LEN // 2 + 1, CACHE_LEN + 1), jax.random.fold_in(part_keys[6], 1), CACHE_LEN // 2 + 1, CACHE_LEN).astype(jnp.int32)
    slots = jax.random.permutation(part_keys[7], RESIDENT).astype(jnp.int32)
    return {"prompt_kv": prompt_kv, "prompt_length": prompt_length, "queries": queries, "new_kv": new_kv, "k_cache": k_cache, "v_cache": v_cache, "lengths": lengths, "slots": slots}


query_scale = 168.0 ** -0.5
negative = -1.0e30


def reference(prompt_kv, prompt_length, queries, new_kv, k_cache, v_cache, lengths, slots):
    position = jnp.arange(PROMPT, dtype=jnp.int32)
    kept = jnp.where((position < prompt_length[0])[:, None, None], prompt_kv, jnp.zeros_like(prompt_kv))
    blocks = kept.reshape(N_SEQ, N_TP, BLOCK, KV_ROWS, HD)
    prompt_owned = jnp.transpose(blocks, (1, 0, 2, 3, 4)).reshape(PROMPT, KV_ROWS, HD)

    rows = jnp.arange(PAIRS, dtype=jnp.int32)
    head_of = rows // RESIDENT
    slot_of = rows % RESIDENT
    match = slots[None, :] == slot_of[:, None]
    sequence = jnp.sum(jnp.where(match, jnp.arange(RESIDENT, dtype=jnp.int32)[None, :], 0), axis=1).astype(jnp.int32)
    grouped = queries.reshape(RESIDENT, KVH, GROUP, HD)
    query_rows = grouped[sequence, head_of].astype(jnp.float32)
    own = new_kv[sequence, head_of]
    own_key = own[:, 0].astype(jnp.float32)
    own_value = own[:, 1].astype(jnp.float32)
    live_len = lengths[sequence]

    scores = jnp.einsum("rgd,rpd->rgp", query_rows, k_cache.astype(jnp.float32)) * query_scale
    own_score = jnp.einsum("rgd,rd->rg", query_rows, own_key) * query_scale
    cache_pos = jnp.arange(CACHE_LEN, dtype=jnp.int32)
    live = cache_pos[None, None, :] < live_len[:, None, None]
    masked = jnp.where(live, scores, negative)
    top = jnp.maximum(jnp.max(masked, axis=2), own_score)
    weights = jnp.where(live, jnp.exp(masked - top[..., None]), 0.0)
    rounded = lax.optimization_barrier(weights.astype(jnp.bfloat16))
    summed = jnp.einsum("rgp,rpd->rgd", rounded.astype(jnp.float32), v_cache.astype(jnp.float32))
    own_weight = jnp.exp(own_score - top)
    total = jnp.sum(weights, axis=2) + own_weight
    summed = summed + own_weight[..., None] * own_value[:, None, :]
    attended = (summed / total[..., None]).astype(jnp.bfloat16).reshape(PAIRS, GROUP * HD)
    return prompt_owned, attended
```

```python
import functools
import jax
import jax.numpy as jnp
from jax import lax
from jax.experimental import pallas as pl
from jax.experimental.pallas import tpu as pltpu
from jax.sharding import PartitionSpec as P

query_scale = 168.0 ** (-0.5)
negative = -1e30

CHUNKS = 4
STEP = 256


def merged(part, axis, combine):
    gathered = jax.tree.map(lambda a: lax.all_gather(a, axis), part)

    def take(source):
        return jax.tree.map(lambda a: lax.dynamic_index_in_dim(a, source, 0, False), gathered)

    return lax.fori_loop(
        1, lax.axis_size(axis), lambda source, state: combine(state, take(source)), take(0)
    )


def combine_parts(first, second):
    upper = jnp.maximum(first[0], second[0])
    scale_one = jnp.exp(first[0] - upper)
    scale_two = jnp.exp(second[0] - upper)
    total = first[1] * scale_one + second[1] * scale_two
    summed = first[2] * scale_one[..., None] + second[2] * scale_two[..., None]
    return (upper, total, summed)


def attend(queries, new_kv, k_cache, v_cache, lengths, slots):
    resident = lengths.shape[0]
    pair_rows = k_cache.shape[0]
    span = k_cache.shape[1]
    width = k_cache.shape[2]
    heads = new_kv.shape[1]
    group = queries.shape[1] // (heads * width)
    rows = lax.axis_index("seq") * pair_rows + jnp.arange(pair_rows, dtype=jnp.int32)
    head_of = rows // resident
    slot_of = rows % resident
    match = slots[None, :] == slot_of[:, None]
    sequence = jnp.sum(jnp.where(match, jnp.arange(resident, dtype=jnp.int32)[None, :], 0), axis=1)
    grouped = queries.reshape(resident, heads, group, width)
    query_rows = grouped[sequence, head_of]
    own = new_kv[sequence, head_of]
    own_key = own[:, 0]
    own_value = own[:, 1].astype(jnp.float32)
    live_len = lengths[sequence]
    scores = (
        jnp.einsum("rgd,rpd->rgp", query_rows, k_cache, preferred_element_type=jnp.float32)
        * query_scale
    )
    own_score = (
        jnp.einsum("rgd,rd->rg", query_rows, own_key, preferred_element_type=jnp.float32)
        * query_scale
    )
    cache_pos = lax.axis_index("tp") * span + jnp.arange(span, dtype=jnp.int32)
    live = cache_pos[None, None, :] < live_len[:, None, None]
    masked = jnp.where(live, scores, negative)
    local_top = jnp.max(masked, axis=2)
    weights = jnp.where(live, jnp.exp(masked - local_top[..., None]), 0.0)
    partial_value = jnp.einsum(
        "rgp,rpd->rgd", weights.astype(jnp.bfloat16), v_cache, preferred_element_type=jnp.float32
    )
    upper, total, summed = merged(
        (local_top, jnp.sum(weights, axis=2), partial_value), "tp", combine_parts
    )
    overall = jnp.maximum(upper, own_score)
    rescale = jnp.exp(upper - overall)
    own_weight = jnp.exp(own_score - overall)
    total = total * rescale + own_weight
    summed = summed * rescale[..., None] + own_weight[..., None] * own_value[:, None, :]
    return (summed / total[..., None]).astype(jnp.bfloat16).reshape(pair_rows, group * width)


def cut_kernel(info, source, piece, *, step):
    first = pl.program_id(0) * step + info[2]
    spot = first + lax.broadcasted_iota(jnp.int32, piece.shape, 0)
    piece[...] = jnp.where(spot < info[1], source[...].reshape(piece.shape), jnp.zeros_like(piece))


def cut(blocks, peer, bound, start, count):
    _, _, rows, width = blocks.shape
    step = min(STEP, count)
    first = start // step
    return pl.pallas_call(
        functools.partial(cut_kernel, step=step),
        grid_spec=pltpu.PrefetchScalarGridSpec(
            num_scalar_prefetch=1,
            grid=(count // step,),
            in_specs=[pl.BlockSpec((step, 1, rows, width), lambda i, info: (first + i, info[0], 0, 0))],
            out_specs=pl.BlockSpec((step, rows, width), lambda i, info: (i, 0, 0)),
        ),
        out_shape=jax.ShapeDtypeStruct((count, rows, width), blocks.dtype),
        cost_estimate=pl.CostEstimate(flops=count * rows * width, bytes_accessed=4 * count * rows * width, transcendentals=0),
        name="cut",
    )(jnp.stack([peer, bound, jnp.int32(start)]), blocks)


def own_kernel(info, source, whole, *, step):
    spot = pl.program_id(0) * step + lax.broadcasted_iota(jnp.int32, whole.shape, 0)
    whole[...] = jnp.where(spot < info[1], source[...].reshape(whole.shape), jnp.zeros_like(whole))


def own_part(blocks, me, bound):
    count, n, rows, width = blocks.shape
    step = min(STEP, count)
    steps = count // step
    return pl.pallas_call(
        functools.partial(own_kernel, step=step),
        grid_spec=pltpu.PrefetchScalarGridSpec(
            num_scalar_prefetch=1,
            grid=(steps,),
            in_specs=[pl.BlockSpec((step, 1, rows, width), lambda i, info: (i, info[0], 0, 0))],
            out_specs=pl.BlockSpec((step, rows, width), lambda i, info: (info[0] * steps + i, 0, 0)),
        ),
        out_shape=jax.ShapeDtypeStruct((n * count, rows, width), blocks.dtype),
        cost_estimate=pl.CostEstimate(flops=count * rows * width, bytes_accessed=4 * count * rows * width, transcendentals=0),
        name="own",
    )(jnp.stack([me, bound]), blocks)


def place_kernel(info, piece, _, whole):
    whole[...] = piece[...]


def place(whole, piece, source, block, start):
    count, rows, width = piece.shape
    step = min(STEP, count)
    steps, first = block // step, start // step
    return pl.pallas_call(
        place_kernel,
        grid_spec=pltpu.PrefetchScalarGridSpec(
            num_scalar_prefetch=1,
            grid=(count // step,),
            in_specs=[
                pl.BlockSpec((step, rows, width), lambda i, info: (i, 0, 0)),
                pl.BlockSpec(memory_space=pl.ANY),
            ],
            out_specs=pl.BlockSpec((step, rows, width), lambda i, info: (info[0] * steps + first + i, 0, 0)),
        ),
        out_shape=jax.ShapeDtypeStruct(whole.shape, whole.dtype),
        input_output_aliases={2: 0},
        cost_estimate=pl.CostEstimate(flops=count * rows * width, bytes_accessed=4 * count * rows * width, transcendentals=0),
        name="place",
    )(jnp.stack([source]), piece, whole)


def per_device(prompt_kv, prompt_length, queries, new_kv, k_cache, v_cache, lengths, slots):
    block, store, width = prompt_kv.shape
    n = lax.axis_size("seq")
    me = lax.axis_index("seq").astype(jnp.int32)
    offset = (me * lax.axis_size("tp") + lax.axis_index("tp")) * block
    bound = prompt_length[0] - offset
    blocks = prompt_kv.reshape(block, n, store // n, width)
    chunks = min(CHUNKS, block // 16)
    size = block // chunks
    moves = []
    for c in range(chunks):
        for d in range(n - 1, 0, -1):
            peer = me ^ d
            piece = cut(blocks, peer, bound, c * size, size)
            got = lax.ppermute(piece, "seq", [(i, i ^ d) for i in range(n)])
            moves.append((got, peer, c * size))
    whole = own_part(blocks, me, bound)
    attended = attend(queries, new_kv, k_cache, v_cache, lengths, slots)
    for got, peer, start in moves:
        whole = place(whole, got, peer, block, start)
    return (whole, attended)


def solution(mesh):
    in_specs = (
        P(("groups", "seq", "tp"), None, None),
        P("groups"),
        P("groups", None),
        P("groups", None, None, None),
        P(("groups", "seq"), "tp", None),
        P(("groups", "seq"), "tp", None),
        P("groups"),
        P("groups"),
    )
    out_specs = (P(("groups", "tp"), "seq", None), P(("groups", "seq"), None))
    return jax.shard_map(
        per_device, mesh=mesh, in_specs=in_specs, out_specs=out_specs, check_vma=False
    )
```

```python
import functools
import math
import jax
import jax.numpy as jnp
from jax import lax
from jax.experimental import pallas as pl
from jax.experimental.pallas import tpu as pltpu
from jax.sharding import PartitionSpec as P

query_scale = 168.0 ** (-0.5)
negative = -1e30

STEP = 256
PART = 64
EARLY = (2, 6, 8, 8, 6)


def merged(part, axis, combine):
    gathered = jax.tree.map(lambda a: lax.all_gather(a, axis), part)

    def take(source):
        return jax.tree.map(lambda a: lax.dynamic_index_in_dim(a, source, 0, False), gathered)

    return lax.fori_loop(
        1, lax.axis_size(axis), lambda source, state: combine(state, take(source)), take(0)
    )


def combine_parts(first, second):
    upper = jnp.maximum(first[0], second[0])
    scale_one = jnp.exp(first[0] - upper)
    scale_two = jnp.exp(second[0] - upper)
    total = first[1] * scale_one + second[1] * scale_two
    summed = first[2] * scale_one[..., None] + second[2] * scale_two[..., None]
    return (upper, total, summed)


def attend(queries, new_kv, k_cache, v_cache, lengths, slots):
    resident = lengths.shape[0]
    pair_rows = k_cache.shape[0]
    span = k_cache.shape[1]
    width = k_cache.shape[2]
    heads = new_kv.shape[1]
    group = queries.shape[1] // (heads * width)
    rows = lax.axis_index("seq") * pair_rows + jnp.arange(pair_rows, dtype=jnp.int32)
    head_of = rows // resident
    slot_of = rows % resident
    match = slots[None, :] == slot_of[:, None]
    sequence = jnp.sum(jnp.where(match, jnp.arange(resident, dtype=jnp.int32)[None, :], 0), axis=1)
    grouped = queries.reshape(resident, heads, group, width)
    query_rows = grouped[sequence, head_of]
    own = new_kv[sequence, head_of]
    own_key = own[:, 0]
    own_value = own[:, 1].astype(jnp.float32)
    live_len = lengths[sequence]
    scores = (
        jnp.einsum("rgd,rpd->rgp", query_rows, k_cache, preferred_element_type=jnp.float32)
        * query_scale
    )
    own_score = (
        jnp.einsum("rgd,rd->rg", query_rows, own_key, preferred_element_type=jnp.float32)
        * query_scale
    )
    cache_pos = lax.axis_index("tp") * span + jnp.arange(span, dtype=jnp.int32)
    live = cache_pos[None, None, :] < live_len[:, None, None]
    masked = jnp.where(live, scores, negative)
    local_top = jnp.max(masked, axis=2)
    weights = jnp.where(live, jnp.exp(masked - local_top[..., None]), 0.0)
    partial_value = jnp.einsum(
        "rgp,rpd->rgd", weights.astype(jnp.bfloat16), v_cache, preferred_element_type=jnp.float32
    )
    upper, total, summed = merged(
        (local_top, jnp.sum(weights, axis=2), partial_value), "tp", combine_parts
    )
    overall = jnp.maximum(upper, own_score)
    rescale = jnp.exp(upper - overall)
    own_weight = jnp.exp(own_score - overall)
    total = total * rescale + own_weight
    summed = summed * rescale[..., None] + own_weight[..., None] * own_value[:, None, :]
    return (summed / total[..., None]).astype(jnp.bfloat16).reshape(pair_rows, group * width)


def cost_of(shape):
    count = math.prod(shape)
    return pl.CostEstimate(flops=count, bytes_accessed=4 * count, transcendentals=0)


def parts_of(count):
    size = max(PART, -(-count // 8))
    return [(at, min(size, count - at)) for at in range(0, count, size)]


def through(jobs):
    steps = []
    for held, reads, writes, source_at, dest_at, fix in jobs:
        for k, (at, size) in enumerate(parts_of(held.shape[0])):
            slot = held.at[pl.ds(at, size)]
            taken = pltpu.make_async_copy(source_at(at, size), slot, reads.at[k])
            put = pltpu.make_async_copy(slot, dest_at(at, size), writes.at[k])
            steps.append((taken, put, fix and functools.partial(fix, at, size)))
    for taken, _, _ in steps:
        taken.start()
    for taken, put, fix in steps:
        taken.wait()
        if fix is not None:
            fix()
        put.start()
    for _, put, _ in steps:
        put.wait()


def clear(held, bound, at, size):
    @pl.when(bound < at + size)
    def _():
        rows = held[pl.ds(at, size)]
        spot = at + lax.broadcasted_iota(jnp.int32, rows.shape, 0)
        held[pl.ds(at, size)] = jnp.where(spot < bound, rows, jnp.zeros_like(rows))


def scratch(shape, dtype):
    count = len(parts_of(shape[0]))
    return [pltpu.VMEM(shape, dtype), pltpu.SemaphoreType.DMA((count,)), pltpu.SemaphoreType.DMA((count,))]


def cut_kernel(info, source, _, piece, held, reads, writes, *, d, start):
    peer = lax.axis_index("seq") ^ d
    through([(
        held,
        reads,
        writes,
        lambda at, size: source.at[pl.ds(start + at, size), peer],
        lambda at, size: piece.at[pl.ds(at, size)],
        functools.partial(clear, held, info[1] - start),
    )])


def cut(info, blocks, d, start, count, after):
    _, _, rows, width = blocks.shape
    return pl.pallas_call(
        functools.partial(cut_kernel, d=d, start=start),
        in_specs=[pl.BlockSpec(memory_space=pltpu.SMEM)] + [pl.BlockSpec(memory_space=pl.ANY)] * 2,
        out_specs=pl.BlockSpec(memory_space=pl.ANY),
        out_shape=jax.ShapeDtypeStruct((count, rows, width), blocks.dtype),
        scratch_shapes=scratch((count, rows, width), blocks.dtype),
        cost_estimate=cost_of((count, rows, width)),
        name="cut",
    )(info, blocks, after)


def lead_kernel(source, _, piece, sem, *, d, start):
    peer = lax.axis_index("seq") ^ d
    copy = pltpu.make_async_copy(source.at[pl.ds(start, piece.shape[0]), peer], piece, sem)
    copy.start()
    copy.wait()


def lead(blocks, d, start, count, after):
    _, _, rows, width = blocks.shape
    return pl.pallas_call(
        functools.partial(lead_kernel, d=d, start=start),
        in_specs=[pl.BlockSpec(memory_space=pl.ANY)] * 2,
        out_specs=pl.BlockSpec(memory_space=pltpu.VMEM),
        out_shape=jax.ShapeDtypeStruct((count, rows, width), blocks.dtype),
        scratch_shapes=[pltpu.SemaphoreType.DMA],
        cost_estimate=cost_of((count, rows, width)),
        name="lead",
    )(blocks, after)


def place_kernel(*refs, spots, block, masked):
    me = lax.axis_index("seq")
    pieces = refs[masked:masked + len(spots)]
    _, whole, *held = refs[masked + len(spots):]
    jobs = []
    for k, (d, start) in enumerate(spots):
        base = (me ^ d) * block + start
        fix = None
        if masked:
            info = refs[0]
            bound = info[1] + (me - (me ^ d)) * info[2] - start
            fix = functools.partial(clear, held[3 * k], bound)
        jobs.append((
            *held[3 * k:3 * k + 3],
            lambda at, size, k=k: pieces[k].at[pl.ds(at, size)],
            lambda at, size, base=base: whole.at[pl.ds(base + at, size)],
            fix,
        ))
    through(jobs)


def place(info, whole, placed, block):
    masked = int(any(start == 0 for _, _, start in placed))
    pieces = [got for got, _, _ in placed]
    return pl.pallas_call(
        functools.partial(place_kernel, spots=[(d, start) for _, d, start in placed], block=block, masked=masked),
        in_specs=[pl.BlockSpec(memory_space=pltpu.SMEM)] * masked
        + [pl.BlockSpec(memory_space=pl.ANY)] * (len(pieces) + 1),
        out_specs=pl.BlockSpec(memory_space=pl.ANY),
        out_shape=jax.ShapeDtypeStruct(whole.shape, whole.dtype),
        scratch_shapes=[x for got in pieces for x in scratch(got.shape, got.dtype)],
        input_output_aliases={masked + len(pieces): 0},
        cost_estimate=cost_of((sum(got.shape[0] for got in pieces), *whole.shape[1:])),
        name="place",
    )(*[info] * masked, *pieces, whole)


def own_kernel(info, source, whole, *, step):
    spot = pl.program_id(0) * step + lax.broadcasted_iota(jnp.int32, whole.shape, 0)
    whole[...] = jnp.where(spot < info[1], source[...].reshape(whole.shape), jnp.zeros_like(whole))


def own_part(info, blocks):
    count, n, rows, width = blocks.shape
    step = min(STEP, count)
    steps = count // step
    return pl.pallas_call(
        functools.partial(own_kernel, step=step),
        grid_spec=pltpu.PrefetchScalarGridSpec(
            num_scalar_prefetch=1,
            grid=(steps,),
            in_specs=[pl.BlockSpec((step, 1, rows, width), lambda i, info: (i, info[0], 0, 0))],
            out_specs=pl.BlockSpec((step, rows, width), lambda i, info: (info[0] * steps + i, 0, 0)),
        ),
        out_shape=jax.ShapeDtypeStruct((n * count, rows, width), blocks.dtype),
        cost_estimate=cost_of((count, rows, width)),
        name="own",
    )(info, blocks)


def plan(n, block):
    unit = block // 32
    if unit < 16 or block % 32:
        return [[(d, 0, block)] for d in range(n - 1, 0, -1)]
    sizes = [unit * share for share in EARLY]
    groups, start = [], 0
    for size in sizes:
        groups += [[(d, start, size)] for d in (range(n - 1, 0, -1) if start == 0 else range(1, n))]
        start += size
    rest = block - start
    groups += [[(d, start, rest)] for d in range(1, n - 2)]
    groups.append([(n - 2, start, rest), (n - 1, start, rest - unit)])
    groups.append([(n - 1, block - unit, unit)])
    return groups


def per_device(prompt_kv, prompt_length, queries, new_kv, k_cache, v_cache, lengths, slots):
    block, store, width = prompt_kv.shape
    n = lax.axis_size("seq")
    me = lax.axis_index("seq").astype(jnp.int32)
    offset = (me * lax.axis_size("tp") + lax.axis_index("tp")) * block
    bound = prompt_length[0] - offset
    blocks = prompt_kv.reshape(block, n, store // n, width)
    info = jnp.stack([me, bound, lax.axis_size("tp") * block])
    groups = []
    after = blocks
    for group in plan(n, block):
        placed = []
        for d, start, size in group:
            if start == 0:
                piece = lead(blocks, d, start, size, after)
            else:
                piece = cut(info, blocks, d, start, size, after)
            after = piece
            placed.append((lax.ppermute(piece, "seq", [(i, i ^ d) for i in range(n)]), d, start))
        groups.append(placed)
    whole = own_part(info, blocks)
    attended = attend(queries, new_kv, k_cache, v_cache, lengths, slots)
    for placed in groups:
        whole = place(info, whole, placed, block)
    return (whole, attended)


def solution(mesh):
    in_specs = (
        P(("groups", "seq", "tp"), None, None),
        P("groups"),
        P("groups", None),
        P("groups", None, None, None),
        P(("groups", "seq"), "tp", None),
        P(("groups", "seq"), "tp", None),
        P("groups"),
        P("groups"),
    )
    out_specs = (P(("groups", "tp"), "seq", None), P(("groups", "seq"), None))
    return jax.shard_map(
        per_device, mesh=mesh, in_specs=in_specs, out_specs=out_specs, check_vma=False
    )
```

```python
import functools
import math
import jax
import jax.numpy as jnp
from jax import lax
from jax.experimental import pallas as pl
from jax.experimental.pallas import tpu as pltpu
from jax.sharding import PartitionSpec as P

query_scale = 168.0 ** (-0.5)
negative = -1e30

STEP = 256
PART = 64
EARLY = (2, 6, 8, 8, 6)


def merged(part, axis, combine):
    gathered = jax.tree.map(lambda a: lax.all_gather(a, axis), part)

    def take(source):
        return jax.tree.map(lambda a: lax.dynamic_index_in_dim(a, source, 0, False), gathered)

    return lax.fori_loop(
        1, lax.axis_size(axis), lambda source, state: combine(state, take(source)), take(0)
    )


def combine_parts(first, second):
    upper = jnp.maximum(first[0], second[0])
    scale_one = jnp.exp(first[0] - upper)
    scale_two = jnp.exp(second[0] - upper)
    total = first[1] * scale_one + second[1] * scale_two
    summed = first[2] * scale_one[..., None] + second[2] * scale_two[..., None]
    return (upper, total, summed)


def attend(queries, new_kv, k_cache, v_cache, lengths, slots):
    resident = lengths.shape[0]
    pair_rows = k_cache.shape[0]
    span = k_cache.shape[1]
    width = k_cache.shape[2]
    heads = new_kv.shape[1]
    group = queries.shape[1] // (heads * width)
    rows = lax.axis_index("seq") * pair_rows + jnp.arange(pair_rows, dtype=jnp.int32)
    head_of = rows // resident
    slot_of = rows % resident
    match = slots[None, :] == slot_of[:, None]
    sequence = jnp.sum(jnp.where(match, jnp.arange(resident, dtype=jnp.int32)[None, :], 0), axis=1)
    grouped = queries.reshape(resident, heads, group, width)
    query_rows = grouped[sequence, head_of]
    own = new_kv[sequence, head_of]
    own_key = own[:, 0]
    own_value = own[:, 1].astype(jnp.float32)
    live_len = lengths[sequence]
    scores = (
        jnp.einsum("rgd,rpd->rgp", query_rows, k_cache, preferred_element_type=jnp.float32)
        * query_scale
    )
    own_score = (
        jnp.einsum("rgd,rd->rg", query_rows, own_key, preferred_element_type=jnp.float32)
        * query_scale
    )
    cache_pos = lax.axis_index("tp") * span + jnp.arange(span, dtype=jnp.int32)
    live = cache_pos[None, None, :] < live_len[:, None, None]
    masked = jnp.where(live, scores, negative)
    local_top = jnp.max(masked, axis=2)
    weights = jnp.where(live, jnp.exp(masked - local_top[..., None]), 0.0)
    partial_value = jnp.einsum(
        "rgp,rpd->rgd", weights.astype(jnp.bfloat16), v_cache, preferred_element_type=jnp.float32
    )
    upper, total, summed = merged(
        (local_top, jnp.sum(weights, axis=2), partial_value), "tp", combine_parts
    )
    overall = jnp.maximum(upper, own_score)
    rescale = jnp.exp(upper - overall)
    own_weight = jnp.exp(own_score - overall)
    total = total * rescale + own_weight
    summed = summed * rescale[..., None] + own_weight[..., None] * own_value[:, None, :]
    return (summed / total[..., None]).astype(jnp.bfloat16).reshape(pair_rows, group * width)


def cost_of(shape):
    count = math.prod(shape)
    return pl.CostEstimate(flops=count, bytes_accessed=4 * count, transcendentals=0)


def parts_of(count):
    size = max(PART, -(-count // 8))
    return [(at, min(size, count - at)) for at in range(0, count, size)]


def through(jobs):
    steps = []
    for held, reads, writes, source_at, dest_at, fix in jobs:
        for k, (at, size) in enumerate(parts_of(held.shape[0])):
            slot = held.at[pl.ds(at, size)]
            taken = pltpu.make_async_copy(source_at(at, size), slot, reads.at[k])
            put = pltpu.make_async_copy(slot, dest_at(at, size), writes.at[k])
            steps.append((taken, put, fix and functools.partial(fix, at, size)))
    for taken, _, _ in steps:
        taken.start()
    for taken, put, fix in steps:
        taken.wait()
        if fix is not None:
            fix()
        put.start()
    for _, put, _ in steps:
        put.wait()


def clear(held, bound, at, size):
    @pl.when(bound < at + size)
    def _():
        rows = held[pl.ds(at, size)]
        spot = at + lax.broadcasted_iota(jnp.int32, rows.shape, 0)
        held[pl.ds(at, size)] = jnp.where(spot < bound, rows, jnp.zeros_like(rows))


def scratch(shape, dtype):
    count = len(parts_of(shape[0]))
    return [pltpu.VMEM(shape, dtype), pltpu.SemaphoreType.DMA((count,)), pltpu.SemaphoreType.DMA((count,))]


def cut_kernel(info, source, _, piece, held, reads, writes, *, d, start):
    peer = lax.axis_index("seq") ^ d
    through([(
        held,
        reads,
        writes,
        lambda at, size: source.at[pl.ds(start + at, size), peer],
        lambda at, size: piece.at[pl.ds(at, size)],
        functools.partial(clear, held, info[1] - start),
    )])


def cut(info, blocks, d, start, count, after):
    _, _, rows, width = blocks.shape
    return pl.pallas_call(
        functools.partial(cut_kernel, d=d, start=start),
        in_specs=[pl.BlockSpec(memory_space=pltpu.SMEM)] + [pl.BlockSpec(memory_space=pl.ANY)] * 2,
        out_specs=pl.BlockSpec(memory_space=pl.ANY),
        out_shape=jax.ShapeDtypeStruct((count, rows, width), blocks.dtype),
        scratch_shapes=scratch((count, rows, width), blocks.dtype),
        cost_estimate=cost_of((count, rows, width)),
        name="cut",
    )(info, blocks, after)


def lead_kernel(source, _, piece, sem, *, d, start):
    peer = lax.axis_index("seq") ^ d
    copy = pltpu.make_async_copy(source.at[pl.ds(start, piece.shape[0]), peer], piece, sem)
    copy.start()
    copy.wait()


def lead(blocks, d, start, count, after):
    _, _, rows, width = blocks.shape
    return pl.pallas_call(
        functools.partial(lead_kernel, d=d, start=start),
        in_specs=[pl.BlockSpec(memory_space=pl.ANY)] * 2,
        out_specs=pl.BlockSpec(memory_space=pltpu.VMEM),
        out_shape=pltpu.VMEM((count, rows, width), blocks.dtype),
        scratch_shapes=[pltpu.SemaphoreType.DMA],
        cost_estimate=cost_of((count, rows, width)),
        name="lead",
    )(blocks, after)


def place_kernel(*refs, spots, block, masked):
    me = lax.axis_index("seq")
    pieces = refs[masked:masked + len(spots)]
    _, whole, *held = refs[masked + len(spots):]
    jobs = []
    for k, (d, start) in enumerate(spots):
        base = (me ^ d) * block + start
        fix = None
        if masked:
            info = refs[0]
            bound = info[1] + (me - (me ^ d)) * info[2] - start
            fix = functools.partial(clear, held[3 * k], bound)
        jobs.append((
            *held[3 * k:3 * k + 3],
            lambda at, size, k=k: pieces[k].at[pl.ds(at, size)],
            lambda at, size, base=base: whole.at[pl.ds(base + at, size)],
            fix,
        ))
    through(jobs)


def place(info, whole, placed, block):
    masked = int(any(start == 0 for _, _, start in placed))
    pieces = [got for got, _, _ in placed]
    return pl.pallas_call(
        functools.partial(place_kernel, spots=[(d, start) for _, d, start in placed], block=block, masked=masked),
        in_specs=[pl.BlockSpec(memory_space=pltpu.SMEM)] * masked
        + [pl.BlockSpec(memory_space=pl.ANY)] * (len(pieces) + 1),
        out_specs=pl.BlockSpec(memory_space=pl.ANY),
        out_shape=jax.ShapeDtypeStruct(whole.shape, whole.dtype),
        scratch_shapes=[x for got in pieces for x in scratch(got.shape, got.dtype)],
        input_output_aliases={masked + len(pieces): 0},
        cost_estimate=cost_of((sum(got.shape[0] for got in pieces), *whole.shape[1:])),
        name="place",
    )(*[info] * masked, *pieces, whole)


def own_kernel(info, source, whole, *, step):
    spot = pl.program_id(0) * step + lax.broadcasted_iota(jnp.int32, whole.shape, 0)
    whole[...] = jnp.where(spot < info[1], source[...].reshape(whole.shape), jnp.zeros_like(whole))


def own_part(info, blocks):
    count, n, rows, width = blocks.shape
    step = min(STEP, count)
    steps = count // step
    return pl.pallas_call(
        functools.partial(own_kernel, step=step),
        grid_spec=pltpu.PrefetchScalarGridSpec(
            num_scalar_prefetch=1,
            grid=(steps,),
            in_specs=[pl.BlockSpec((step, 1, rows, width), lambda i, info: (i, info[0], 0, 0))],
            out_specs=pl.BlockSpec((step, rows, width), lambda i, info: (info[0] * steps + i, 0, 0)),
        ),
        out_shape=jax.ShapeDtypeStruct((n * count, rows, width), blocks.dtype),
        cost_estimate=cost_of((count, rows, width)),
        name="own",
    )(info, blocks)


def plan(n, block):
    unit = block // 32
    if unit < 16 or block % 32:
        return [[(d, 0, block)] for d in range(n - 1, 0, -1)]
    sizes = [unit * share for share in EARLY]
    groups, start = [], 0
    for size in sizes:
        groups += [[(d, start, size)] for d in (range(n - 1, 0, -1) if start == 0 else range(1, n))]
        start += size
    rest = block - start
    groups += [[(d, start, rest)] for d in range(1, n - 2)]
    groups.append([(n - 2, start, rest), (n - 1, start, rest - unit)])
    groups.append([(n - 1, block - unit, unit)])
    return groups


def per_device(prompt_kv, prompt_length, queries, new_kv, k_cache, v_cache, lengths, slots):
    block, store, width = prompt_kv.shape
    n = lax.axis_size("seq")
    me = lax.axis_index("seq").astype(jnp.int32)
    offset = (me * lax.axis_size("tp") + lax.axis_index("tp")) * block
    bound = prompt_length[0] - offset
    blocks = prompt_kv.reshape(block, n, store // n, width)
    info = jnp.stack([me, bound, lax.axis_size("tp") * block])
    groups = []
    after = blocks
    for group in plan(n, block):
        placed = []
        for d, start, size in group:
            if start == 0:
                piece = lead(blocks, d, start, size, after)
            else:
                piece = cut(info, blocks, d, start, size, after)
            after = piece
            placed.append((lax.ppermute(piece, "seq", [(i, i ^ d) for i in range(n)]), d, start))
        groups.append(placed)
    whole = own_part(info, blocks)
    attended = attend(queries, new_kv, k_cache, v_cache, lengths, slots)
    for placed in groups:
        whole = place(info, whole, placed, block)
    return (whole, attended)


def solution(mesh):
    in_specs = (
        P(("groups", "seq", "tp"), None, None),
        P("groups"),
        P("groups", None),
        P("groups", None, None, None),
        P(("groups", "seq"), "tp", None),
        P(("groups", "seq"), "tp", None),
        P("groups"),
        P("groups"),
    )
    out_specs = (P(("groups", "tp"), "seq", None), P(("groups", "seq"), None))
    return jax.shard_map(
        per_device, mesh=mesh, in_specs=in_specs, out_specs=out_specs, check_vma=False
    )
```

```python
import functools
import math
import jax
import jax.numpy as jnp
from jax import lax
from jax.experimental import pallas as pl
from jax.experimental.pallas import tpu as pltpu
from jax.sharding import PartitionSpec as P

query_scale = 168.0 ** (-0.5)
negative = -1e30

STEP = 256
PART = 128
EARLY = (2, 6, 8, 8, 6)


def merged(part, axis, combine):
    gathered = jax.tree.map(lambda a: lax.all_gather(a, axis), part)

    def take(source):
        return jax.tree.map(lambda a: lax.dynamic_index_in_dim(a, source, 0, False), gathered)

    return lax.fori_loop(
        1, lax.axis_size(axis), lambda source, state: combine(state, take(source)), take(0)
    )


def combine_parts(first, second):
    upper = jnp.maximum(first[0], second[0])
    scale_one = jnp.exp(first[0] - upper)
    scale_two = jnp.exp(second[0] - upper)
    total = first[1] * scale_one + second[1] * scale_two
    summed = first[2] * scale_one[..., None] + second[2] * scale_two[..., None]
    return (upper, total, summed)


def attend(queries, new_kv, k_cache, v_cache, lengths, slots):
    resident = lengths.shape[0]
    pair_rows = k_cache.shape[0]
    span = k_cache.shape[1]
    width = k_cache.shape[2]
    heads = new_kv.shape[1]
    group = queries.shape[1] // (heads * width)
    rows = lax.axis_index("seq") * pair_rows + jnp.arange(pair_rows, dtype=jnp.int32)
    head_of = rows // resident
    slot_of = rows % resident
    match = slots[None, :] == slot_of[:, None]
    sequence = jnp.sum(jnp.where(match, jnp.arange(resident, dtype=jnp.int32)[None, :], 0), axis=1)
    grouped = queries.reshape(resident, heads, group, width)
    query_rows = grouped[sequence, head_of]
    own = new_kv[sequence, head_of]
    own_key = own[:, 0]
    own_value = own[:, 1].astype(jnp.float32)
    live_len = lengths[sequence]
    scores = (
        jnp.einsum("rgd,rpd->rgp", query_rows, k_cache, preferred_element_type=jnp.float32)
        * query_scale
    )
    own_score = (
        jnp.einsum("rgd,rd->rg", query_rows, own_key, preferred_element_type=jnp.float32)
        * query_scale
    )
    cache_pos = lax.axis_index("tp") * span + jnp.arange(span, dtype=jnp.int32)
    live = cache_pos[None, None, :] < live_len[:, None, None]
    masked = jnp.where(live, scores, negative)
    local_top = jnp.max(masked, axis=2)
    weights = jnp.where(live, jnp.exp(masked - local_top[..., None]), 0.0)
    partial_value = jnp.einsum(
        "rgp,rpd->rgd", weights.astype(jnp.bfloat16), v_cache, preferred_element_type=jnp.float32
    )
    upper, total, summed = merged(
        (local_top, jnp.sum(weights, axis=2), partial_value), "tp", combine_parts
    )
    overall = jnp.maximum(upper, own_score)
    rescale = jnp.exp(upper - overall)
    own_weight = jnp.exp(own_score - overall)
    total = total * rescale + own_weight
    summed = summed * rescale[..., None] + own_weight[..., None] * own_value[:, None, :]
    return (summed / total[..., None]).astype(jnp.bfloat16).reshape(pair_rows, group * width)


def cost_of(shape):
    count = math.prod(shape)
    return pl.CostEstimate(flops=count, bytes_accessed=4 * count, transcendentals=0)


def parts_of(count, size):
    return [(at, min(size, count - at)) for at in range(0, count, size)]


def through(jobs, part):
    steps = []
    for held, reads, writes, source_at, dest_at, fix in jobs:
        for k, (at, size) in enumerate(parts_of(held.shape[0], part)):
            slot = held.at[pl.ds(at, size)]
            taken = pltpu.make_async_copy(source_at(at, size), slot, reads.at[k])
            put = pltpu.make_async_copy(slot, dest_at(at, size), writes.at[k])
            steps.append((taken, put, fix and functools.partial(fix, at, size)))
    for taken, _, _ in steps:
        taken.start()
    for taken, put, fix in steps:
        taken.wait()
        if fix is not None:
            fix()
        put.start()
    for _, put, _ in steps:
        put.wait()


def clear(held, bound, at, size):
    @pl.when(bound < at + size)
    def _():
        rows = held[pl.ds(at, size)]
        spot = at + lax.broadcasted_iota(jnp.int32, rows.shape, 0)
        held[pl.ds(at, size)] = jnp.where(spot < bound, rows, jnp.zeros_like(rows))


def scratch(shape, dtype, part):
    count = len(parts_of(shape[0], part))
    return [pltpu.VMEM(shape, dtype), pltpu.SemaphoreType.DMA((count,)), pltpu.SemaphoreType.DMA((count,))]


def cut_kernel(info, source, _, piece, held, reads, writes, *, d, start):
    peer = lax.axis_index("seq") ^ d
    through([(
        held,
        reads,
        writes,
        lambda at, size: source.at[pl.ds(start + at, size), peer],
        lambda at, size: piece.at[pl.ds(at, size)],
        functools.partial(clear, held, info[1] - start),
    )], PART)


def cut(info, blocks, d, start, count, after):
    _, _, rows, width = blocks.shape
    return pl.pallas_call(
        functools.partial(cut_kernel, d=d, start=start),
        in_specs=[pl.BlockSpec(memory_space=pltpu.SMEM)] + [pl.BlockSpec(memory_space=pl.ANY)] * 2,
        out_specs=pl.BlockSpec(memory_space=pl.ANY),
        out_shape=jax.ShapeDtypeStruct((count, rows, width), blocks.dtype),
        scratch_shapes=scratch((count, rows, width), blocks.dtype, PART),
        cost_estimate=cost_of((count, rows, width)),
        name="cut",
    )(info, blocks, after)


def lead_kernel(source, _, piece, sem, *, d, start):
    peer = lax.axis_index("seq") ^ d
    copy = pltpu.make_async_copy(source.at[pl.ds(start, piece.shape[0]), peer], piece, sem)
    copy.start()
    copy.wait()


def lead(blocks, d, start, count, after):
    _, _, rows, width = blocks.shape
    return pl.pallas_call(
        functools.partial(lead_kernel, d=d, start=start),
        in_specs=[pl.BlockSpec(memory_space=pl.ANY)] * 2,
        out_specs=pl.BlockSpec(memory_space=pltpu.VMEM),
        out_shape=pltpu.VMEM((count, rows, width), blocks.dtype),
        scratch_shapes=[pltpu.SemaphoreType.DMA],
        cost_estimate=cost_of((count, rows, width)),
        name="lead",
    )(blocks, after)


def place_kernel(*refs, spots, block, masked):
    me = lax.axis_index("seq")
    pieces = refs[masked:masked + len(spots)]
    _, whole, *held = refs[masked + len(spots):]
    jobs = []
    for k, (d, start) in enumerate(spots):
        base = (me ^ d) * block + start
        fix = None
        if masked:
            info = refs[0]
            bound = info[1] + (me - (me ^ d)) * info[2] - start
            fix = functools.partial(clear, held[3 * k], bound)
        jobs.append((
            *held[3 * k:3 * k + 3],
            lambda at, size, k=k: pieces[k].at[pl.ds(at, size)],
            lambda at, size, base=base: whole.at[pl.ds(base + at, size)],
            fix,
        ))
    through(jobs, block)


def place(info, whole, placed, block):
    masked = int(any(start == 0 for _, _, start in placed))
    pieces = [got for got, _, _ in placed]
    return pl.pallas_call(
        functools.partial(place_kernel, spots=[(d, start) for _, d, start in placed], block=block, masked=masked),
        in_specs=[pl.BlockSpec(memory_space=pltpu.SMEM)] * masked
        + [pl.BlockSpec(memory_space=pl.ANY)] * (len(pieces) + 1),
        out_specs=pl.BlockSpec(memory_space=pl.ANY),
        out_shape=jax.ShapeDtypeStruct(whole.shape, whole.dtype),
        scratch_shapes=[x for got in pieces for x in scratch(got.shape, got.dtype, block)],
        input_output_aliases={masked + len(pieces): 0},
        cost_estimate=cost_of((sum(got.shape[0] for got in pieces), *whole.shape[1:])),
        name="place",
    )(*[info] * masked, *pieces, whole)


def own_kernel(info, source, whole, *, step):
    spot = pl.program_id(0) * step + lax.broadcasted_iota(jnp.int32, whole.shape, 0)
    whole[...] = jnp.where(spot < info[1], source[...].reshape(whole.shape), jnp.zeros_like(whole))


def own_part(info, blocks):
    count, n, rows, width = blocks.shape
    step = min(STEP, count)
    steps = count // step
    return pl.pallas_call(
        functools.partial(own_kernel, step=step),
        grid_spec=pltpu.PrefetchScalarGridSpec(
            num_scalar_prefetch=1,
            grid=(steps,),
            in_specs=[pl.BlockSpec((step, 1, rows, width), lambda i, info: (i, info[0], 0, 0))],
            out_specs=pl.BlockSpec((step, rows, width), lambda i, info: (info[0] * steps + i, 0, 0)),
        ),
        out_shape=jax.ShapeDtypeStruct((n * count, rows, width), blocks.dtype),
        cost_estimate=cost_of((count, rows, width)),
        name="own",
    )(info, blocks)


def plan(n, block):
    unit = block // 32
    if unit < 16 or block % 32:
        return [[(d, 0, block)] for d in range(n - 1, 0, -1)]
    sizes = [unit * share for share in EARLY]
    groups, start = [], 0
    for size in sizes:
        groups += [[(d, start, size)] for d in (range(n - 1, 0, -1) if start == 0 else range(1, n))]
        start += size
    rest = block - start
    groups += [[(d, start, rest)] for d in range(1, n - 2)]
    groups.append([(n - 2, start, rest), (n - 1, start, rest - unit), (n - 1, block - unit, unit)])
    return groups


def per_device(prompt_kv, prompt_length, queries, new_kv, k_cache, v_cache, lengths, slots):
    block, store, width = prompt_kv.shape
    n = lax.axis_size("seq")
    me = lax.axis_index("seq").astype(jnp.int32)
    offset = (me * lax.axis_size("tp") + lax.axis_index("tp")) * block
    bound = prompt_length[0] - offset
    blocks = prompt_kv.reshape(block, n, store // n, width)
    info = jnp.stack([me, bound, lax.axis_size("tp") * block])
    groups = []
    after = blocks
    for group in plan(n, block):
        placed = []
        for d, start, size in group:
            if start == 0:
                piece = lead(blocks, d, start, size, after)
            else:
                piece = cut(info, blocks, d, start, size, after)
            after = piece
            placed.append((lax.ppermute(piece, "seq", [(i, i ^ d) for i in range(n)]), d, start))
        groups.append(placed)
    whole = own_part(info, blocks)
    attended = attend(queries, new_kv, k_cache, v_cache, lengths, slots)
    for placed in groups:
        whole = place(info, whole, placed, block)
    return (whole, attended)


def solution(mesh):
    in_specs = (
        P(("groups", "seq", "tp"), None, None),
        P("groups"),
        P("groups", None),
        P("groups", None, None, None),
        P(("groups", "seq"), "tp", None),
        P(("groups", "seq"), "tp", None),
        P("groups"),
        P("groups"),
    )
    out_specs = (P(("groups", "tp"), "seq", None), P(("groups", "seq"), None))
    return jax.shard_map(
        per_device, mesh=mesh, in_specs=in_specs, out_specs=out_specs, check_vma=False
    )
```

```python
import functools
import math
import jax
import jax.numpy as jnp
from jax import lax
from jax.experimental import pallas as pl
from jax.experimental.pallas import tpu as pltpu
from jax.sharding import PartitionSpec as P

query_scale = 168.0 ** (-0.5)
negative = -1e30

STEP = 256
PART = 128
EARLY = (2, 6, 8, 8, 6)


def merged(part, axis, combine):
    gathered = jax.tree.map(lambda a: lax.all_gather(a, axis), part)

    def take(source):
        return jax.tree.map(lambda a: lax.dynamic_index_in_dim(a, source, 0, False), gathered)

    return lax.fori_loop(
        1, lax.axis_size(axis), lambda source, state: combine(state, take(source)), take(0)
    )


def combine_parts(first, second):
    upper = jnp.maximum(first[0], second[0])
    scale_one = jnp.exp(first[0] - upper)
    scale_two = jnp.exp(second[0] - upper)
    total = first[1] * scale_one + second[1] * scale_two
    summed = first[2] * scale_one[..., None] + second[2] * scale_two[..., None]
    return (upper, total, summed)


def attend(queries, new_kv, k_cache, v_cache, lengths, slots):
    resident = lengths.shape[0]
    pair_rows = k_cache.shape[0]
    span = k_cache.shape[1]
    width = k_cache.shape[2]
    heads = new_kv.shape[1]
    group = queries.shape[1] // (heads * width)
    rows = lax.axis_index("seq") * pair_rows + jnp.arange(pair_rows, dtype=jnp.int32)
    head_of = rows // resident
    slot_of = rows % resident
    match = slots[None, :] == slot_of[:, None]
    sequence = jnp.sum(jnp.where(match, jnp.arange(resident, dtype=jnp.int32)[None, :], 0), axis=1)
    grouped = queries.reshape(resident, heads, group, width)
    query_rows = grouped[sequence, head_of]
    own = new_kv[sequence, head_of]
    own_key = own[:, 0]
    own_value = own[:, 1].astype(jnp.float32)
    live_len = lengths[sequence]
    scores = (
        jnp.einsum("rgd,rpd->rgp", query_rows, k_cache, preferred_element_type=jnp.float32)
        * query_scale
    )
    own_score = (
        jnp.einsum("rgd,rd->rg", query_rows, own_key, preferred_element_type=jnp.float32)
        * query_scale
    )
    cache_pos = lax.axis_index("tp") * span + jnp.arange(span, dtype=jnp.int32)
    live = cache_pos[None, None, :] < live_len[:, None, None]
    masked = jnp.where(live, scores, negative)
    local_top = jnp.max(masked, axis=2)
    weights = jnp.where(live, jnp.exp(masked - local_top[..., None]), 0.0)
    partial_value = jnp.einsum(
        "rgp,rpd->rgd", weights.astype(jnp.bfloat16), v_cache, preferred_element_type=jnp.float32
    )
    upper, total, summed = merged(
        (local_top, jnp.sum(weights, axis=2), partial_value), "tp", combine_parts
    )
    overall = jnp.maximum(upper, own_score)
    rescale = jnp.exp(upper - overall)
    own_weight = jnp.exp(own_score - overall)
    total = total * rescale + own_weight
    summed = summed * rescale[..., None] + own_weight[..., None] * own_value[:, None, :]
    return (summed / total[..., None]).astype(jnp.bfloat16).reshape(pair_rows, group * width)


def cost_of(shape):
    count = math.prod(shape)
    return pl.CostEstimate(flops=count, bytes_accessed=4 * count, transcendentals=0)


def parts_of(count, size):
    return [(at, min(size, count - at)) for at in range(0, count, size)]


def through(jobs, part):
    steps = []
    for held, reads, writes, source_at, dest_at, fix in jobs:
        for k, (at, size) in enumerate(parts_of(held.shape[0], part)):
            slot = held.at[pl.ds(at, size)]
            taken = pltpu.make_async_copy(source_at(at, size), slot, reads.at[k])
            put = pltpu.make_async_copy(slot, dest_at(at, size), writes.at[k])
            steps.append((taken, put, fix and functools.partial(fix, at, size)))
    for taken, _, _ in steps:
        taken.start()
    for taken, put, fix in steps:
        taken.wait()
        if fix is not None:
            fix()
        put.start()
    for _, put, _ in steps:
        put.wait()


def clear(held, bound, at, size):
    @pl.when(bound < at + size)
    def _():
        rows = held[pl.ds(at, size)]
        spot = at + lax.broadcasted_iota(jnp.int32, rows.shape, 0)
        held[pl.ds(at, size)] = jnp.where(spot < bound, rows, jnp.zeros_like(rows))


def scratch(shape, dtype, part):
    count = len(parts_of(shape[0], part))
    return [pltpu.VMEM(shape, dtype), pltpu.SemaphoreType.DMA((count,)), pltpu.SemaphoreType.DMA((count,))]


def cut_kernel(info, source, _, *refs, spots):
    me = lax.axis_index("seq")
    pieces, held = refs[:len(spots)], refs[len(spots):]
    jobs = []
    for k, (d, start, _) in enumerate(spots):
        peer = me ^ d
        jobs.append((
            *held[3 * k:3 * k + 3],
            lambda at, size, start=start, peer=peer: source.at[pl.ds(start + at, size), peer],
            lambda at, size, k=k: pieces[k].at[pl.ds(at, size)],
            functools.partial(clear, held[3 * k], info[1] - start),
        ))
    through(jobs, PART)


def cut(info, blocks, spots, after):
    _, _, rows, width = blocks.shape
    shapes = [(size, rows, width) for _, _, size in spots]
    return pl.pallas_call(
        functools.partial(cut_kernel, spots=spots),
        in_specs=[pl.BlockSpec(memory_space=pltpu.SMEM)] + [pl.BlockSpec(memory_space=pl.ANY)] * 2,
        out_specs=[pl.BlockSpec(memory_space=pl.ANY)] * len(spots),
        out_shape=[jax.ShapeDtypeStruct(shape, blocks.dtype) for shape in shapes],
        scratch_shapes=[x for shape in shapes for x in scratch(shape, blocks.dtype, PART)],
        cost_estimate=cost_of((sum(size for _, _, size in spots), rows, width)),
        name="cut",
    )(info, blocks, after)


def lead_kernel(source, _, piece, sem, *, d, start):
    peer = lax.axis_index("seq") ^ d
    copy = pltpu.make_async_copy(source.at[pl.ds(start, piece.shape[0]), peer], piece, sem)
    copy.start()
    copy.wait()


def lead(blocks, d, start, count, after):
    _, _, rows, width = blocks.shape
    return pl.pallas_call(
        functools.partial(lead_kernel, d=d, start=start),
        in_specs=[pl.BlockSpec(memory_space=pl.ANY)] * 2,
        out_specs=pl.BlockSpec(memory_space=pltpu.VMEM),
        out_shape=pltpu.VMEM((count, rows, width), blocks.dtype),
        scratch_shapes=[pltpu.SemaphoreType.DMA],
        cost_estimate=cost_of((count, rows, width)),
        name="lead",
    )(blocks, after)


def place_kernel(*refs, spots, block, masked):
    me = lax.axis_index("seq")
    pieces = refs[masked:masked + len(spots)]
    _, whole, *held = refs[masked + len(spots):]
    jobs = []
    for k, (d, start) in enumerate(spots):
        base = (me ^ d) * block + start
        fix = None
        if masked:
            info = refs[0]
            bound = info[1] + (me - (me ^ d)) * info[2] - start
            fix = functools.partial(clear, held[3 * k], bound)
        jobs.append((
            *held[3 * k:3 * k + 3],
            lambda at, size, k=k: pieces[k].at[pl.ds(at, size)],
            lambda at, size, base=base: whole.at[pl.ds(base + at, size)],
            fix,
        ))
    through(jobs, block)


def place(info, whole, placed, block):
    masked = int(any(start == 0 for _, _, start in placed))
    pieces = [got for got, _, _ in placed]
    return pl.pallas_call(
        functools.partial(place_kernel, spots=[(d, start) for _, d, start in placed], block=block, masked=masked),
        in_specs=[pl.BlockSpec(memory_space=pltpu.SMEM)] * masked
        + [pl.BlockSpec(memory_space=pl.ANY)] * (len(pieces) + 1),
        out_specs=pl.BlockSpec(memory_space=pl.ANY),
        out_shape=jax.ShapeDtypeStruct(whole.shape, whole.dtype),
        scratch_shapes=[x for got in pieces for x in scratch(got.shape, got.dtype, block)],
        input_output_aliases={masked + len(pieces): 0},
        cost_estimate=cost_of((sum(got.shape[0] for got in pieces), *whole.shape[1:])),
        name="place",
    )(*[info] * masked, *pieces, whole)


def own_kernel(info, source, whole, *, step):
    spot = pl.program_id(0) * step + lax.broadcasted_iota(jnp.int32, whole.shape, 0)
    whole[...] = jnp.where(spot < info[1], source[...].reshape(whole.shape), jnp.zeros_like(whole))


def own_part(info, blocks):
    count, n, rows, width = blocks.shape
    step = min(STEP, count)
    steps = count // step
    return pl.pallas_call(
        functools.partial(own_kernel, step=step),
        grid_spec=pltpu.PrefetchScalarGridSpec(
            num_scalar_prefetch=1,
            grid=(steps,),
            in_specs=[pl.BlockSpec((step, 1, rows, width), lambda i, info: (i, info[0], 0, 0))],
            out_specs=pl.BlockSpec((step, rows, width), lambda i, info: (info[0] * steps + i, 0, 0)),
        ),
        out_shape=jax.ShapeDtypeStruct((n * count, rows, width), blocks.dtype),
        cost_estimate=cost_of((count, rows, width)),
        name="own",
    )(info, blocks)


def plan(n, block):
    unit = block // 32
    if unit < 16 or block % 32:
        rounds = [[(d, 0, block)] for d in range(n - 1, 0, -1)]
        return rounds, rounds
    rounds, start = [], 0
    for share in EARLY:
        size = unit * share
        rounds.append([(d, start, size) for d in (range(1, n) if start else range(n - 1, 0, -1))])
        start += size
    rest = block - start
    near = [(d, start, rest) for d in range(1, n - 2)]
    last = [(n - 2, start, rest), (n - 1, start, rest - unit), (n - 1, block - unit, unit)]
    return rounds + [near + last], rounds[:-1] + [rounds[-1] + near, last]


def per_device(prompt_kv, prompt_length, queries, new_kv, k_cache, v_cache, lengths, slots):
    block, store, width = prompt_kv.shape
    n = lax.axis_size("seq")
    me = lax.axis_index("seq").astype(jnp.int32)
    offset = (me * lax.axis_size("tp") + lax.axis_index("tp")) * block
    bound = prompt_length[0] - offset
    blocks = prompt_kv.reshape(block, n, store // n, width)
    info = jnp.stack([me, bound, lax.axis_size("tp") * block])
    rounds, groups = plan(n, block)
    got = {}
    after = blocks
    for spots in rounds:
        if spots[0][1] == 0:
            pieces = []
            for spot in spots:
                after = lead(blocks, *spot, after)
                pieces.append(after)
        else:
            pieces = cut(info, blocks, spots, after)
            after = pieces[-1]
        for (d, start, _), piece in zip(spots, pieces):
            got[d, start] = lax.ppermute(piece, "seq", [(i, i ^ d) for i in range(n)])
    whole = own_part(info, blocks)
    attended = attend(queries, new_kv, k_cache, v_cache, lengths, slots)
    for spots in groups:
        whole = place(info, whole, [(got[d, start], d, start) for d, start, _ in spots], block)
    return (whole, attended)


def solution(mesh):
    in_specs = (
        P(("groups", "seq", "tp"), None, None),
        P("groups"),
        P("groups", None),
        P("groups", None, None, None),
        P(("groups", "seq"), "tp", None),
        P(("groups", "seq"), "tp", None),
        P("groups"),
        P("groups"),
    )
    out_specs = (P(("groups", "tp"), "seq", None), P(("groups", "seq"), None))
    return jax.shard_map(
        per_device, mesh=mesh, in_specs=in_specs, out_specs=out_specs, check_vma=False
    )
```

```python
import functools
import math
import jax
import jax.numpy as jnp
from jax import lax
from jax.experimental import pallas as pl
from jax.experimental.pallas import tpu as pltpu
from jax.sharding import PartitionSpec as P

query_scale = 168.0 ** (-0.5)
negative = -1e30

STEP = 256
PART = 128
EARLY = (2, 9, 10, 9)


def merged(part, axis, combine):
    gathered = jax.tree.map(lambda a: lax.all_gather(a, axis), part)

    def take(source):
        return jax.tree.map(lambda a: lax.dynamic_index_in_dim(a, source, 0, False), gathered)

    return lax.fori_loop(
        1, lax.axis_size(axis), lambda source, state: combine(state, take(source)), take(0)
    )


def combine_parts(first, second):
    upper = jnp.maximum(first[0], second[0])
    scale_one = jnp.exp(first[0] - upper)
    scale_two = jnp.exp(second[0] - upper)
    total = first[1] * scale_one + second[1] * scale_two
    summed = first[2] * scale_one[..., None] + second[2] * scale_two[..., None]
    return (upper, total, summed)


def attend(queries, new_kv, k_cache, v_cache, lengths, slots):
    resident = lengths.shape[0]
    pair_rows = k_cache.shape[0]
    span = k_cache.shape[1]
    width = k_cache.shape[2]
    heads = new_kv.shape[1]
    group = queries.shape[1] // (heads * width)
    rows = lax.axis_index("seq") * pair_rows + jnp.arange(pair_rows, dtype=jnp.int32)
    head_of = rows // resident
    slot_of = rows % resident
    match = slots[None, :] == slot_of[:, None]
    sequence = jnp.sum(jnp.where(match, jnp.arange(resident, dtype=jnp.int32)[None, :], 0), axis=1)
    grouped = queries.reshape(resident, heads, group, width)
    query_rows = grouped[sequence, head_of]
    own = new_kv[sequence, head_of]
    own_key = own[:, 0]
    own_value = own[:, 1].astype(jnp.float32)
    live_len = lengths[sequence]
    scores = (
        jnp.einsum("rgd,rpd->rgp", query_rows, k_cache, preferred_element_type=jnp.float32)
        * query_scale
    )
    own_score = (
        jnp.einsum("rgd,rd->rg", query_rows, own_key, preferred_element_type=jnp.float32)
        * query_scale
    )
    cache_pos = lax.axis_index("tp") * span + jnp.arange(span, dtype=jnp.int32)
    live = cache_pos[None, None, :] < live_len[:, None, None]
    masked = jnp.where(live, scores, negative)
    local_top = jnp.max(masked, axis=2)
    weights = jnp.where(live, jnp.exp(masked - local_top[..., None]), 0.0)
    partial_value = jnp.einsum(
        "rgp,rpd->rgd", weights.astype(jnp.bfloat16), v_cache, preferred_element_type=jnp.float32
    )
    upper, total, summed = merged(
        (local_top, jnp.sum(weights, axis=2), partial_value), "tp", combine_parts
    )
    overall = jnp.maximum(upper, own_score)
    rescale = jnp.exp(upper - overall)
    own_weight = jnp.exp(own_score - overall)
    total = total * rescale + own_weight
    summed = summed * rescale[..., None] + own_weight[..., None] * own_value[:, None, :]
    return (summed / total[..., None]).astype(jnp.bfloat16).reshape(pair_rows, group * width)


def cost_of(shape):
    count = math.prod(shape)
    return pl.CostEstimate(flops=count, bytes_accessed=4 * count, transcendentals=0)


def parts_of(count, size):
    return [(at, min(size, count - at)) for at in range(0, count, size)]


def through(jobs, part):
    steps = []
    for held, reads, writes, source_at, dest_at, fix in jobs:
        for k, (at, size) in enumerate(parts_of(held.shape[0], part)):
            slot = held.at[pl.ds(at, size)]
            taken = pltpu.make_async_copy(source_at(at, size), slot, reads.at[k])
            put = pltpu.make_async_copy(slot, dest_at(at, size), writes.at[k])
            steps.append((taken, put, fix and functools.partial(fix, at, size)))
    for taken, _, _ in steps:
        taken.start()
    for taken, put, fix in steps:
        taken.wait()
        if fix is not None:
            fix()
        put.start()
    for _, put, _ in steps:
        put.wait()


def clear(held, bound, at, size):
    @pl.when(bound < at + size)
    def _():
        rows = held[pl.ds(at, size)]
        spot = at + lax.broadcasted_iota(jnp.int32, rows.shape, 0)
        held[pl.ds(at, size)] = jnp.where(spot < bound, rows, jnp.zeros_like(rows))


def scratch(shape, dtype, part):
    count = len(parts_of(shape[0], part))
    return [pltpu.VMEM(shape, dtype), pltpu.SemaphoreType.DMA((count,)), pltpu.SemaphoreType.DMA((count,))]


def cut_kernel(info, source, _, *refs, spots):
    me = lax.axis_index("seq")
    pieces, held = refs[:len(spots)], refs[len(spots):]
    jobs = []
    for k, (d, start, _) in enumerate(spots):
        peer = me ^ d
        jobs.append((
            *held[3 * k:3 * k + 3],
            lambda at, size, start=start, peer=peer: source.at[pl.ds(start + at, size), peer],
            lambda at, size, k=k: pieces[k].at[pl.ds(at, size)],
            functools.partial(clear, held[3 * k], info[1] - start),
        ))
    through(jobs, PART)


def cut(info, blocks, spots, after):
    _, _, rows, width = blocks.shape
    shapes = [(size, rows, width) for _, _, size in spots]
    return pl.pallas_call(
        functools.partial(cut_kernel, spots=spots),
        in_specs=[pl.BlockSpec(memory_space=pltpu.SMEM)] + [pl.BlockSpec(memory_space=pl.ANY)] * 2,
        out_specs=[pl.BlockSpec(memory_space=pl.ANY)] * len(spots),
        out_shape=[jax.ShapeDtypeStruct(shape, blocks.dtype) for shape in shapes],
        scratch_shapes=[x for shape in shapes for x in scratch(shape, blocks.dtype, PART)],
        cost_estimate=cost_of((sum(size for _, _, size in spots), rows, width)),
        name="cut",
    )(info, blocks, after)


def lead_kernel(source, _, piece, sem, *, d, start):
    peer = lax.axis_index("seq") ^ d
    copy = pltpu.make_async_copy(source.at[pl.ds(start, piece.shape[0]), peer], piece, sem)
    copy.start()
    copy.wait()


def lead(blocks, d, start, count, after):
    _, _, rows, width = blocks.shape
    return pl.pallas_call(
        functools.partial(lead_kernel, d=d, start=start),
        in_specs=[pl.BlockSpec(memory_space=pl.ANY)] * 2,
        out_specs=pl.BlockSpec(memory_space=pltpu.VMEM),
        out_shape=pltpu.VMEM((count, rows, width), blocks.dtype),
        scratch_shapes=[pltpu.SemaphoreType.DMA],
        cost_estimate=cost_of((count, rows, width)),
        name="lead",
    )(blocks, after)


def place_kernel(*refs, spots, block, masked):
    me = lax.axis_index("seq")
    pieces = refs[masked:masked + len(spots)]
    _, whole, *held = refs[masked + len(spots):]
    jobs = []
    for k, (d, start) in enumerate(spots):
        base = (me ^ d) * block + start
        fix = None
        if masked:
            info = refs[0]
            bound = info[1] + (me - (me ^ d)) * info[2] - start
            fix = functools.partial(clear, held[3 * k], bound)
        jobs.append((
            *held[3 * k:3 * k + 3],
            lambda at, size, k=k: pieces[k].at[pl.ds(at, size)],
            lambda at, size, base=base: whole.at[pl.ds(base + at, size)],
            fix,
        ))
    through(jobs, block)


def place(info, whole, placed, block):
    masked = int(any(start == 0 for _, _, start in placed))
    pieces = [got for got, _, _ in placed]
    return pl.pallas_call(
        functools.partial(place_kernel, spots=[(d, start) for _, d, start in placed], block=block, masked=masked),
        in_specs=[pl.BlockSpec(memory_space=pltpu.SMEM)] * masked
        + [pl.BlockSpec(memory_space=pl.ANY)] * (len(pieces) + 1),
        out_specs=pl.BlockSpec(memory_space=pl.ANY),
        out_shape=jax.ShapeDtypeStruct(whole.shape, whole.dtype),
        scratch_shapes=[x for got in pieces for x in scratch(got.shape, got.dtype, block)],
        input_output_aliases={masked + len(pieces): 0},
        cost_estimate=cost_of((sum(got.shape[0] for got in pieces), *whole.shape[1:])),
        name="place",
    )(*[info] * masked, *pieces, whole)


def own_kernel(info, source, whole, *, step):
    spot = pl.program_id(0) * step + lax.broadcasted_iota(jnp.int32, whole.shape, 0)
    whole[...] = jnp.where(spot < info[1], source[...].reshape(whole.shape), jnp.zeros_like(whole))


def own_part(info, blocks):
    count, n, rows, width = blocks.shape
    step = min(STEP, count)
    steps = count // step
    return pl.pallas_call(
        functools.partial(own_kernel, step=step),
        grid_spec=pltpu.PrefetchScalarGridSpec(
            num_scalar_prefetch=1,
            grid=(steps,),
            in_specs=[pl.BlockSpec((step, 1, rows, width), lambda i, info: (i, info[0], 0, 0))],
            out_specs=pl.BlockSpec((step, rows, width), lambda i, info: (info[0] * steps + i, 0, 0)),
        ),
        out_shape=jax.ShapeDtypeStruct((n * count, rows, width), blocks.dtype),
        cost_estimate=cost_of((count, rows, width)),
        name="own",
    )(info, blocks)


def plan(n, block):
    unit = block // 32
    if unit < 16 or block % 32:
        rounds = [[(d, 0, block)] for d in range(n - 1, 0, -1)]
        return rounds, rounds
    rounds, start = [], 0
    for share in EARLY:
        size = unit * share
        rounds.append([(d, start, size) for d in (range(1, n) if start else range(n - 1, 0, -1))])
        start += size
    rest = block - start
    near = [(d, start, rest) for d in range(1, n - 2)]
    last = [(n - 2, start, rest), (n - 1, start, rest - unit), (n - 1, block - unit, unit)]
    return rounds + [near + last], rounds[:-1] + [rounds[-1] + near, last]


def per_device(prompt_kv, prompt_length, queries, new_kv, k_cache, v_cache, lengths, slots):
    block, store, width = prompt_kv.shape
    n = lax.axis_size("seq")
    me = lax.axis_index("seq").astype(jnp.int32)
    offset = (me * lax.axis_size("tp") + lax.axis_index("tp")) * block
    bound = prompt_length[0] - offset
    blocks = prompt_kv.reshape(block, n, store // n, width)
    info = jnp.stack([me, bound, lax.axis_size("tp") * block])
    rounds, groups = plan(n, block)
    got = {}
    after = blocks
    for spots in rounds:
        if spots[0][1] == 0:
            pieces = []
            for spot in spots:
                after = lead(blocks, *spot, after)
                pieces.append(after)
        else:
            pieces = cut(info, blocks, spots, after)
            after = pieces[-1]
        for (d, start, _), piece in zip(spots, pieces):
            got[d, start] = lax.ppermute(piece, "seq", [(i, i ^ d) for i in range(n)])
    whole = own_part(info, blocks)
    attended = attend(queries, new_kv, k_cache, v_cache, lengths, slots)
    for spots in groups:
        whole = place(info, whole, [(got[d, start], d, start) for d, start, _ in spots], block)
    return (whole, attended)


def solution(mesh):
    in_specs = (
        P(("groups", "seq", "tp"), None, None),
        P("groups"),
        P("groups", None),
        P("groups", None, None, None),
        P(("groups", "seq"), "tp", None),
        P(("groups", "seq"), "tp", None),
        P("groups"),
        P("groups"),
    )
    out_specs = (P(("groups", "tp"), "seq", None), P(("groups", "seq"), None))
    return jax.shard_map(
        per_device, mesh=mesh, in_specs=in_specs, out_specs=out_specs, check_vma=False
    )
```

```python
import functools
import math
import jax
import jax.numpy as jnp
from jax import lax
from jax.experimental import pallas as pl
from jax.experimental.pallas import tpu as pltpu
from jax.sharding import PartitionSpec as P

query_scale = 168.0 ** (-0.5)
negative = -1e30

STEP = 256
PART = 128
EARLY = (2, 18, 10)


def merged(part, axis, combine):
    gathered = jax.tree.map(lambda a: lax.all_gather(a, axis), part)

    def take(source):
        return jax.tree.map(lambda a: lax.dynamic_index_in_dim(a, source, 0, False), gathered)

    return lax.fori_loop(
        1, lax.axis_size(axis), lambda source, state: combine(state, take(source)), take(0)
    )


def combine_parts(first, second):
    upper = jnp.maximum(first[0], second[0])
    scale_one = jnp.exp(first[0] - upper)
    scale_two = jnp.exp(second[0] - upper)
    total = first[1] * scale_one + second[1] * scale_two
    summed = first[2] * scale_one[..., None] + second[2] * scale_two[..., None]
    return (upper, total, summed)


def attend(queries, new_kv, k_cache, v_cache, lengths, slots):
    resident = lengths.shape[0]
    pair_rows = k_cache.shape[0]
    span = k_cache.shape[1]
    width = k_cache.shape[2]
    heads = new_kv.shape[1]
    group = queries.shape[1] // (heads * width)
    rows = lax.axis_index("seq") * pair_rows + jnp.arange(pair_rows, dtype=jnp.int32)
    head_of = rows // resident
    slot_of = rows % resident
    match = slots[None, :] == slot_of[:, None]
    sequence = jnp.sum(jnp.where(match, jnp.arange(resident, dtype=jnp.int32)[None, :], 0), axis=1)
    grouped = queries.reshape(resident, heads, group, width)
    query_rows = grouped[sequence, head_of]
    own = new_kv[sequence, head_of]
    own_key = own[:, 0]
    own_value = own[:, 1].astype(jnp.float32)
    live_len = lengths[sequence]
    scores = (
        jnp.einsum("rgd,rpd->rgp", query_rows, k_cache, preferred_element_type=jnp.float32)
        * query_scale
    )
    own_score = (
        jnp.einsum("rgd,rd->rg", query_rows, own_key, preferred_element_type=jnp.float32)
        * query_scale
    )
    cache_pos = lax.axis_index("tp") * span + jnp.arange(span, dtype=jnp.int32)
    live = cache_pos[None, None, :] < live_len[:, None, None]
    masked = jnp.where(live, scores, negative)
    local_top = jnp.max(masked, axis=2)
    weights = jnp.where(live, jnp.exp(masked - local_top[..., None]), 0.0)
    partial_value = jnp.einsum(
        "rgp,rpd->rgd", weights.astype(jnp.bfloat16), v_cache, preferred_element_type=jnp.float32
    )
    upper, total, summed = merged(
        (local_top, jnp.sum(weights, axis=2), partial_value), "tp", combine_parts
    )
    overall = jnp.maximum(upper, own_score)
    rescale = jnp.exp(upper - overall)
    own_weight = jnp.exp(own_score - overall)
    total = total * rescale + own_weight
    summed = summed * rescale[..., None] + own_weight[..., None] * own_value[:, None, :]
    return (summed / total[..., None]).astype(jnp.bfloat16).reshape(pair_rows, group * width)


def cost_of(shape):
    count = math.prod(shape)
    return pl.CostEstimate(flops=count, bytes_accessed=4 * count, transcendentals=0)


def parts_of(count, size):
    return [(at, min(size, count - at)) for at in range(0, count, size)]


def through(jobs, part):
    steps = []
    for held, reads, writes, source_at, dest_at, fix in jobs:
        for k, (at, size) in enumerate(parts_of(held.shape[0], part)):
            slot = held.at[pl.ds(at, size)]
            taken = pltpu.make_async_copy(source_at(at, size), slot, reads.at[k])
            put = pltpu.make_async_copy(slot, dest_at(at, size), writes.at[k])
            steps.append((taken, put, fix and functools.partial(fix, at, size)))
    for taken, _, _ in steps:
        taken.start()
    for taken, put, fix in steps:
        taken.wait()
        if fix is not None:
            fix()
        put.start()
    for _, put, _ in steps:
        put.wait()


def clear(held, bound, at, size):
    @pl.when(bound < at + size)
    def _():
        rows = held[pl.ds(at, size)]
        spot = at + lax.broadcasted_iota(jnp.int32, rows.shape, 0)
        held[pl.ds(at, size)] = jnp.where(spot < bound, rows, jnp.zeros_like(rows))


def scratch(shape, dtype, part):
    count = len(parts_of(shape[0], part))
    return [pltpu.VMEM(shape, dtype), pltpu.SemaphoreType.DMA((count,)), pltpu.SemaphoreType.DMA((count,))]


def cut_kernel(info, source, _, *refs, spots):
    me = lax.axis_index("seq")
    pieces, held = refs[:len(spots)], refs[len(spots):]
    jobs = []
    for k, (d, start, _) in enumerate(spots):
        peer = me ^ d
        jobs.append((
            *held[3 * k:3 * k + 3],
            lambda at, size, start=start, peer=peer: source.at[pl.ds(start + at, size), peer],
            lambda at, size, k=k: pieces[k].at[pl.ds(at, size)],
            functools.partial(clear, held[3 * k], info[1] - start),
        ))
    through(jobs, PART)


def cut(info, blocks, spots, after):
    _, _, rows, width = blocks.shape
    shapes = [(size, rows, width) for _, _, size in spots]
    return pl.pallas_call(
        functools.partial(cut_kernel, spots=spots),
        in_specs=[pl.BlockSpec(memory_space=pltpu.SMEM)] + [pl.BlockSpec(memory_space=pl.ANY)] * 2,
        out_specs=[pl.BlockSpec(memory_space=pl.ANY)] * len(spots),
        out_shape=[jax.ShapeDtypeStruct(shape, blocks.dtype) for shape in shapes],
        scratch_shapes=[x for shape in shapes for x in scratch(shape, blocks.dtype, PART)],
        cost_estimate=cost_of((sum(size for _, _, size in spots), rows, width)),
        name="cut",
    )(info, blocks, after)


def lead_kernel(source, _, piece, sem, *, d, start):
    peer = lax.axis_index("seq") ^ d
    copy = pltpu.make_async_copy(source.at[pl.ds(start, piece.shape[0]), peer], piece, sem)
    copy.start()
    copy.wait()


def lead(blocks, d, start, count, after):
    _, _, rows, width = blocks.shape
    return pl.pallas_call(
        functools.partial(lead_kernel, d=d, start=start),
        in_specs=[pl.BlockSpec(memory_space=pl.ANY)] * 2,
        out_specs=pl.BlockSpec(memory_space=pltpu.VMEM),
        out_shape=pltpu.VMEM((count, rows, width), blocks.dtype),
        scratch_shapes=[pltpu.SemaphoreType.DMA],
        cost_estimate=cost_of((count, rows, width)),
        name="lead",
    )(blocks, after)


def place_kernel(*refs, spots, block, masked):
    me = lax.axis_index("seq")
    pieces = refs[masked:masked + len(spots)]
    _, whole, *held = refs[masked + len(spots):]
    jobs = []
    for k, (d, start) in enumerate(spots):
        base = (me ^ d) * block + start
        fix = None
        if masked:
            info = refs[0]
            bound = info[1] + (me - (me ^ d)) * info[2] - start
            fix = functools.partial(clear, held[3 * k], bound)
        jobs.append((
            *held[3 * k:3 * k + 3],
            lambda at, size, k=k: pieces[k].at[pl.ds(at, size)],
            lambda at, size, base=base: whole.at[pl.ds(base + at, size)],
            fix,
        ))
    through(jobs, block)


def place(info, whole, placed, block):
    masked = int(any(start == 0 for _, _, start in placed))
    pieces = [got for got, _, _ in placed]
    return pl.pallas_call(
        functools.partial(place_kernel, spots=[(d, start) for _, d, start in placed], block=block, masked=masked),
        in_specs=[pl.BlockSpec(memory_space=pltpu.SMEM)] * masked
        + [pl.BlockSpec(memory_space=pl.ANY)] * (len(pieces) + 1),
        out_specs=pl.BlockSpec(memory_space=pl.ANY),
        out_shape=jax.ShapeDtypeStruct(whole.shape, whole.dtype),
        scratch_shapes=[x for got in pieces for x in scratch(got.shape, got.dtype, block)],
        input_output_aliases={masked + len(pieces): 0},
        cost_estimate=cost_of((sum(got.shape[0] for got in pieces), *whole.shape[1:])),
        name="place",
    )(*[info] * masked, *pieces, whole)


def own_kernel(info, source, whole, *, step):
    spot = pl.program_id(0) * step + lax.broadcasted_iota(jnp.int32, whole.shape, 0)
    whole[...] = jnp.where(spot < info[1], source[...].reshape(whole.shape), jnp.zeros_like(whole))


def own_part(info, blocks):
    count, n, rows, width = blocks.shape
    step = min(STEP, count)
    steps = count // step
    return pl.pallas_call(
        functools.partial(own_kernel, step=step),
        grid_spec=pltpu.PrefetchScalarGridSpec(
            num_scalar_prefetch=1,
            grid=(steps,),
            in_specs=[pl.BlockSpec((step, 1, rows, width), lambda i, info: (i, info[0], 0, 0))],
            out_specs=pl.BlockSpec((step, rows, width), lambda i, info: (info[0] * steps + i, 0, 0)),
        ),
        out_shape=jax.ShapeDtypeStruct((n * count, rows, width), blocks.dtype),
        cost_estimate=cost_of((count, rows, width)),
        name="own",
    )(info, blocks)


def plan(n, block):
    unit = block // 32
    if unit < 16 or block % 32:
        rounds = [[(d, 0, block)] for d in range(n - 1, 0, -1)]
        return rounds, rounds
    rounds, start = [], 0
    for share in EARLY:
        size = unit * share
        rounds.append([(d, start, size) for d in (range(1, n) if start else range(n - 1, 0, -1))])
        start += size
    rest = block - start
    near = [(d, start, rest) for d in range(1, n - 2)]
    last = [(n - 2, start, rest), (n - 1, start, rest - unit), (n - 1, block - unit, unit)]
    return rounds + [near + last], rounds[:-1] + [rounds[-1] + near, last]


def per_device(prompt_kv, prompt_length, queries, new_kv, k_cache, v_cache, lengths, slots):
    block, store, width = prompt_kv.shape
    n = lax.axis_size("seq")
    me = lax.axis_index("seq").astype(jnp.int32)
    offset = (me * lax.axis_size("tp") + lax.axis_index("tp")) * block
    bound = prompt_length[0] - offset
    blocks = prompt_kv.reshape(block, n, store // n, width)
    info = jnp.stack([me, bound, lax.axis_size("tp") * block])
    rounds, groups = plan(n, block)
    got = {}
    after = blocks
    for spots in rounds:
        if spots[0][1] == 0:
            pieces = []
            for spot in spots:
                after = lead(blocks, *spot, after)
                pieces.append(after)
        else:
            pieces = cut(info, blocks, spots, after)
            after = pieces[-1]
        for (d, start, _), piece in zip(spots, pieces):
            got[d, start] = lax.ppermute(piece, "seq", [(i, i ^ d) for i in range(n)])
    whole = own_part(info, blocks)
    attended = attend(queries, new_kv, k_cache, v_cache, lengths, slots)
    for spots in groups:
        whole = place(info, whole, [(got[d, start], d, start) for d, start, _ in spots], block)
    return (whole, attended)


def solution(mesh):
    in_specs = (
        P(("groups", "seq", "tp"), None, None),
        P("groups"),
        P("groups", None),
        P("groups", None, None, None),
        P(("groups", "seq"), "tp", None),
        P(("groups", "seq"), "tp", None),
        P("groups"),
        P("groups"),
    )
    out_specs = (P(("groups", "tp"), "seq", None), P(("groups", "seq"), None))
    return jax.shard_map(
        per_device, mesh=mesh, in_specs=in_specs, out_specs=out_specs, check_vma=False
    )
```
